32 devices in a mesh: member: 2 (over x), gx: 8 (over z, y), gy: 2 (over core).
Axes of the slice: x: 2, y: 2, z: 4, core: 2. Of those that a mesh axis runs over, the one named last changes fastest.
Arguments:
- conc: float32 [66, 4, 64, 256], P(None, None, ('member', 'gx'), 'gy'), parts along dimension 2, may hold values from 0.001 to 30
- winds: float32 [2, 4, 64, 256], P(None, None, ('member', 'gx'), 'gy'), parts along dimension 2, may hold values from -0.9 to 0.9
- diffusivity: float32 [3, 64, 256], P(None, ('member', 'gx'), 'gy'), parts along dimension 1, may hold values from 0.1 to 10
- emission: float32 [66, 64, 256], P(None, ('member', 'gx'), 'gy'), parts along dimension 1, may hold values from 0.1 to 1
- photo_rate: float32 [66], replicated, may hold values from 0.05 to 1
Outputs:
- conc_next: float32 [66, 4, 64, 256], P(None, None, ('member', 'gx'), 'gy'), parts along dimension 2
The draws below stay inside these ranges and needn't reach their ends.
There are 2 independent parts, one for each index of `member`. The reference program is written for one: setup_inputs(seed, part) draws one part's arguments, and reference() takes and returns one part's arrays. A program takes and returns all parts, laid end to end along the dimension named above; an argument that names none is the same for every part. Nothing has to cross between parts.
All inputs are finite; a program needn't handle non-finite values.
Results may differ from the reference program's by a relative error of at most 0.00002.
Values sent between devices are 32-bit elements; how exact they have to be, the bound alone decides.
A program may use at most 64 MiB of HBM per device.

```python
import math
import jax
import jax.numpy as jnp
from jax import lax

SPEC = 66
LEV = 4
NX = 32
NY = 256


def draw_conc(key, part):
    base_key = jax.random.fold_in(key, 11)
    faint_key = jax.random.fold_in(key, 13)
    peak_key = jax.random.fold_in(key, 14)
    spike_key = jax.random.fold_in(key, 15)
    plume_key = jax.random.fold_in(key, 16)
    shape = (SPEC, LEV, NX, NY)
    rough = jnp.exp(jax.random.uniform(base_key, shape, jnp.float32, jnp.log(0.2), jnp.log(2.0)))
    faint = jnp.exp(jax.random.uniform(faint_key, shape, jnp.float32, jnp.log(0.001), jnp.log(0.01)))
    peak = jnp.exp(jax.random.uniform(peak_key, shape, jnp.float32, jnp.log(2.0), jnp.log(10.0)))
    share = 0.05
    spike = jax.random.uniform(spike_key, shape, jnp.float32) < share
    plumes = jnp.where(spike, peak, faint)
    order = jnp.arange(SPEC)
    plume_species = ((jax.random.uniform(plume_key, (SPEC,), jnp.float32) < 0.5) | (order == 1)) & (order > 0)
    ramp = 1.0 + 2.0 * jnp.arange(NX, dtype=jnp.float32) / NX
    values = jnp.where(plume_species[:, None, None, None], plumes, rough)
    values = values * ramp[None, None, :, None]
    return values.astype(jnp.float32)


def block_levels(own_key, shape, shards, low, largest):
    def one(dim, parts):
        steps = jax.random.uniform(jax.random.fold_in(jax.random.fold_in(own_key, 6), dim), (parts,), jnp.float32, low / len(shards), largest / len(shards))
        return jnp.repeat(jnp.exp(steps), shape[dim] // parts).reshape((-1,) + (1,) * (len(shape) - dim - 1))

    factor_of = one(*shards[0])
    for cut in shards[1:]:
        factor_of = factor_of * one(*cut)
    return factor_of


def setup_inputs(seed: int = 0, part: int = 0) -> dict:
    seeds = jax.random.split(jax.random.key(seed), 6)
    own_keys = jax.random.split(jax.random.fold_in(seeds[5], part), 6)
    conc = draw_conc(jax.random.fold_in(jax.random.fold_in(seeds[5], part), 71), part)
    winds = jnp.clip(jax.random.uniform(own_keys[1], (2, LEV, NX, NY), jnp.float32, -0.9, 0.9) * block_levels(own_keys[1], (2, LEV, NX, NY), ((2, 8), (3, 2)), -0.4, 0.0), -0.9, 0.9)
    diffusivity = jnp.clip(jnp.exp(math.log(10.0) - 4.6051702 * jax.random.uniform(own_keys[2], (LEV - 1, NX, NY), jnp.float32) ** block_levels(own_keys[2], (LEV - 1, NX, NY), ((1, 8), (2, 2)), -0.2, 0.2)), 0.1, 10.0)
    emission = jnp.clip(jnp.exp(math.log(1.0) - 2.3025851 * jax.random.uniform(own_keys[3], (SPEC, NX, NY), jnp.float32) ** block_levels(own_keys[3], (SPEC, NX, NY), ((1, 8), (2, 2)), -0.2, 0.2)), 0.1, 1.0)
    photo_rate = jnp.clip(jnp.exp(jax.random.uniform(seeds[4], (SPEC,), jnp.float32, math.log(0.05), math.log(1.0))), 0.05, 1.0)
    return dict(conc=conc, winds=winds, diffusivity=diffusivity, emission=emission, photo_rate=photo_rate)


BETAS = (1.0 / 3.0, 0.5, 1.0)


def flux_div(field, courant, axis):
    count = field.shape[axis] - 6

    def cut(arr, start):
        return lax.slice_in_dim(arr, start, start + count + 1, axis=axis)

    face = 0.5 * (cut(courant, 2) + cut(courant, 3))
    mean = (37.0 * (cut(field, 2) + cut(field, 3)) - 8.0 * (cut(field, 1) + cut(field, 4)) + (cut(field, 0) + cut(field, 5))) / 60.0
    spread = (10.0 * (cut(field, 3) - cut(field, 2)) - 5.0 * (cut(field, 4) - cut(field, 1)) + (cut(field, 5) - cut(field, 0))) / 60.0
    flux = face * mean - jnp.abs(face) * spread
    return lax.slice_in_dim(flux, 1, count + 1, axis=axis) - lax.slice_in_dim(flux, 0, count, axis=axis)


def advance(padded, wind_east, wind_north, start, beta):
    dx = flux_div(padded, wind_east, 2)
    inner_x = padded[:, :, 3:-3, :]
    partial_x = inner_x - beta * dx
    dy = flux_div(partial_x, wind_north, 3)
    return start + (partial_x[:, :, :, 3:-3] - inner_x[:, :, :, 3:-3]) - beta * dy


def vertical_mix(fixed, diffusivity, emission):
    levels = fixed.shape[1]
    zero = jnp.zeros_like(diffusivity[:1])
    lower = jnp.concatenate([zero, diffusivity], axis=0)
    upper = jnp.concatenate([diffusivity, zero], axis=0)
    diag = 1.0 + lower + upper
    right = fixed.at[:, 0].add(emission)
    ratio = [None] * levels
    value = [None] * levels
    ratio[0] = -upper[0] / diag[0]
    value[0] = right[:, 0] / diag[0]
    for lev in range(1, levels):
        pivot = diag[lev] + lower[lev] * ratio[lev - 1]
        ratio[lev] = -upper[lev] / pivot
        value[lev] = (right[:, lev] + lower[lev] * value[lev - 1]) / pivot
    result = [None] * levels
    result[levels - 1] = value[levels - 1]
    for lev in range(levels - 2, -1, -1):
        result[lev] = value[lev] - ratio[lev] * result[lev + 1]
    return jnp.stack(result, axis=1)


def photolysis(mixed, photo_rate):
    levels = mixed.shape[1]
    absorber = mixed[0]
    above = jnp.cumsum(absorber[::-1], axis=0)[::-1] - 0.5 * absorber
    column = above / levels
    rate = photo_rate[:, None, None, None] * jnp.exp(-0.5 * column)[None]
    return mixed * jnp.exp(-rate)


def reference(conc, winds, diffusivity, emission, photo_rate):
    margin = ((0, 0), (0, 0), (3, 3), (3, 3))
    padded_wind = jnp.pad(winds, margin)
    wind_east = padded_wind[0][None]
    wind_north = padded_wind[1][None][:, :, 3:-3, :]
    state = conc
    for beta in BETAS:
        state = advance(jnp.pad(state, margin), wind_east, wind_north, conc, beta)
    net = jnp.sum(state, axis=(1, 2, 3))
    positive = jnp.maximum(state, 0.0)
    total = jnp.sum(positive, axis=(1, 2, 3))
    fixed = positive * (net / total)[:, None, None, None]
    mixed = vertical_mix(fixed, diffusivity, emission)
    return photolysis(mixed, photo_rate)
```

```python
import functools

import jax
import jax.numpy as jnp
from jax import lax
from jax.experimental import pallas as pl
from jax.experimental.pallas import tpu as pltpu
from jax.sharding import PartitionSpec as P

BETAS = (1.0 / 3.0, 0.5, 1.0)
SUB = 8
LANES = 128
PAD = 3


def stencil_weights(km, kp):
    def face(k):
        k = k / 60.0
        a = jnp.abs(k)
        return (
            k + a,
            -8.0 * k - 5.0 * a,
            37.0 * k + 10.0 * a,
            37.0 * k - 10.0 * a,
            -8.0 * k + 5.0 * a,
            k - a,
        )

    m, p = face(km), face(kp)
    return [-m[0]] + [p[j] - m[j + 1] for j in range(5)] + [p[5]]


def kernel(dims, conc_ref, wind_ref, diff_ref, emis_ref, rate_ref, out_ref,
           send, state0, state_a, state_b, result, back, wsend, wrecv, cbuf, wx, wy,
           stat, stats, ratio_ref, prate, coef,
           in_send, in_recv, w_send, w_recv, out_send, out_recv, s_send, s_recv):
    spec, lev, rows, halves, n, tiles, groups, per_dev = dims
    per = n // lev
    targets = lev * groups
    nx = (n // halves) * rows
    my_gx, my_gy = lax.axis_index("gx"), lax.axis_index("gy")
    me = my_gx * halves + my_gy
    my_lev = me // per
    my_group = (me % per + 2 * per - 2 * (my_lev % 2)) % per
    active = my_group < groups

    def owner(level, group):
        return level * per + (group + 2 * (level % 2)) % per

    def where_is(dev):
        return {"gx": dev // halves, "gy": dev % halves}

    barrier = pltpu.get_barrier_semaphore()

    def greet(k, carry):
        pl.semaphore_signal(barrier, inc=1, device_id=where_is((me + k) % n),
                            device_id_type=pl.DeviceIdType.MESH)
        return carry

    lax.fori_loop(1, n, greet, 0)

    stride = lev * rows
    for lv in range(lev):
        wsend[lv, 0:rows, :] = wind_ref[pl.ds(lv * rows, rows), :]
        wsend[lv, rows:2 * rows, :] = wind_ref[pl.ds((lev + lv) * rows, rows), :]
    for t in range(tiles):
        have = max(0, min(SUB, spec - t * SUB))
        for lv in range(lev):
            for r in range(rows):
                if have < SUB:
                    send[lv, t, r, :, :] = jnp.zeros((SUB, LANES), jnp.float32)
                if have > 0:
                    send[lv, t, r, 0:have, :] = conc_ref[
                        pl.ds(t * SUB * stride + lv * rows + r, have, stride=stride), :]

    pl.semaphore_wait(barrier, n - 1)

    def deliver(src, dst, dev, s_sem, r_sem):
        @pl.when(dev == me)
        def _():
            pltpu.make_async_copy(src, dst, r_sem).start()

        @pl.when(dev != me)
        def _():
            pltpu.make_async_remote_copy(
                src_ref=src, dst_ref=dst, send_sem=s_sem, recv_sem=r_sem,
                device_id=where_is(dev), device_id_type=pl.DeviceIdType.MESH).start()

    def sent(src, dev, s_sem):
        @pl.when(dev != me)
        def _():
            pltpu.make_async_copy(src, src, s_sem).wait()

    def landed(dst, r_sem):
        pltpu.make_async_copy(dst, dst, r_sem).wait()

    def target(k):
        j = (k + me) % targets
        return j, j // groups, j % groups

    def send_winds(k, carry):
        j, level, group = target(k)
        deliver(wsend.at[level], wrecv.at[me], owner(level, group), w_send.at[j], w_recv.at[me])
        return carry

    lax.fori_loop(0, targets, send_winds, 0)
    for t in range(per_dev):

        def send_tile(k, carry):
            j, level, group = target(k)
            deliver(send.at[level, group * per_dev + t],
                    state0.at[t, my_gy, pl.ds(PAD + my_gx * rows, rows)],
                    owner(level, group), in_send.at[j, t], in_recv.at[me, t])
            return carry

        lax.fori_loop(0, targets, send_tile, 0)

    sub = lax.broadcasted_iota(jnp.int32, (SUB, LANES), 0)
    lane = lax.broadcasted_iota(jnp.int32, (SUB, LANES), 1)
    for t in range(tiles):
        tile = jnp.zeros((SUB, LANES), jnp.float32)
        for i in range(SUB):
            if t * SUB + i < spec:
                tile = jnp.where(sub == i, rate_ref[t * SUB + i], tile)
        prate[pl.ds(t * SUB, SUB), :] = tile
    ks = [diff_ref[pl.ds(lv * rows, rows), :] for lv in range(lev - 1)]
    zero = jnp.zeros((rows, LANES), jnp.float32)
    lower = [zero] + ks
    upper = ks + [zero]
    prev = None
    for lv in range(lev):
        pivot = 1.0 + lower[lv] + upper[lv]
        if lv:
            pivot = pivot + lower[lv] * prev
        inv = 1.0 / pivot
        prev = -upper[lv] * inv
        coef[0, pl.ds(lv * rows, rows), :] = inv
        coef[1, pl.ds(lv * rows, rows), :] = lower[lv]
        coef[2, pl.ds(lv * rows, rows), :] = -prev

    @pl.when(active)
    def _():
        blank = jnp.zeros((PAD, SUB, LANES), jnp.float32)
        for t in range(per_dev):
            for h in range(halves):
                state0[t, h, 0:PAD] = blank
                state0[t, h, PAD + nx:2 * PAD + nx] = blank
        for h in range(halves):
            for buf in (state_a, state_b):
                buf[h, 0:PAD] = blank
                buf[h, PAD + nx:2 * PAD + nx] = blank
            for c in range(2):
                cbuf[c, h, 0:SUB, :] = jnp.zeros((SUB, LANES), jnp.float32)
                cbuf[c, h, SUB + nx:2 * SUB + nx, :] = jnp.zeros((SUB, LANES), jnp.float32)

        def wind_in(k, carry):
            landed(wrecv.at[k], w_recv.at[k])
            return carry

        lax.fori_loop(0, n, wind_in, 0)
        for dev in range(n):
            gx, h = dev // halves, dev % halves
            for c in range(2):
                cbuf[c, h, SUB + gx * rows:SUB + (gx + 1) * rows, :] = (
                    wrecv[dev, c * rows:(c + 1) * rows, :])
        for x0 in range(0, nx, SUB):
            for h in range(halves):
                here = cbuf[0, h, SUB + x0:SUB + x0 + SUB, :]
                left = cbuf[0, h, SUB + x0 - 1:SUB + x0 - 1 + SUB, :]
                right = cbuf[0, h, SUB + x0 + 1:SUB + x0 + 1 + SUB, :]
                for j, w in enumerate(stencil_weights(0.5 * (left + here), 0.5 * (here + right))):
                    wx[j, h, x0:x0 + SUB, :] = w
            cy = [cbuf[1, h, SUB + x0:SUB + x0 + SUB, :] for h in range(halves)]
            zer = jnp.zeros((SUB, LANES), jnp.float32)
            for h in range(halves):
                nxt = pltpu.roll(cy[h + 1], LANES - 1, 1) if h + 1 < halves else zer
                prv = pltpu.roll(cy[h - 1], 1, 1) if h > 0 else zer
                up = jnp.where(lane < LANES - 1, pltpu.roll(cy[h], LANES - 1, 1), nxt)
                down = jnp.where(lane >= 1, pltpu.roll(cy[h], 1, 1), prv)
                ws = stencil_weights(0.5 * (down + cy[h]), 0.5 * (cy[h] + up))
                for j, w in enumerate(ws):
                    d = j - 3
                    if d > 0 and h == halves - 1:
                        w = jnp.where(lane < LANES - d, w, 0.0)
                    if d < 0 and h == 0:
                        w = jnp.where(lane >= -d, w, 0.0)
                    wy[j, h, x0:x0 + SUB, :] = w

        def stage(t, src, dst, beta, x, sums):
            partial, change = [], []
            for h in range(halves):
                acc = None
                for j in range(7):
                    term = wx[j, h, pl.ds(x, 1), :] * src(h, x + j)
                    acc = term if acc is None else acc + term
                acc = beta * acc
                change.append(acc)
                partial.append(src(h, x + PAD) - acc)
            acc = [wy[3, h, pl.ds(x, 1), :] * partial[h] for h in range(halves)]
            for d in (1, 2, 3):
                up = [pltpu.roll(p, LANES - d, 1) for p in partial]
                down = [pltpu.roll(p, d, 1) for p in partial]
                for h in range(halves):
                    u = up[h] if h == halves - 1 else jnp.where(lane < LANES - d, up[h], up[h + 1])
                    w = down[h] if h == 0 else jnp.where(lane >= d, down[h], down[h - 1])
                    acc[h] = acc[h] + wy[3 + d, h, pl.ds(x, 1), :] * u
                    acc[h] = acc[h] + wy[3 - d, h, pl.ds(x, 1), :] * w
            for h in range(halves):
                new = state0[t, h, x + PAD] - change[h] - beta * acc[h]
                dst(h, x, new)
                if sums is not None:
                    sums = (sums[0] + new, sums[1] + jnp.maximum(new, 0.0))
            return sums

        def put_a(h, x, v):
            state_a[h, x + PAD] = v

        def put_b(h, x, v):
            state_b[h, x + PAD] = v

        stat[...] = jnp.zeros((SUB, LANES), jnp.float32)
        for t in range(per_dev):

            def tile_in(k, carry):
                landed(state0.at[t, k % halves, pl.ds(PAD + (k // halves) * rows, rows)],
                       in_recv.at[k, t])
                return carry

            lax.fori_loop(0, n, tile_in, 0)

            def put_r(h, x, v):
                result[t, h, x] = v

            @pl.loop(0, nx, unroll=2)
            def _(x):
                stage(t, lambda h, i: state0[t, h, i], put_a, BETAS[0], x, None)

            @pl.loop(0, nx, unroll=2)
            def _(x):
                stage(t, lambda h, i: state_a[h, i], put_b, BETAS[1], x, None)

            z = jnp.zeros((SUB, LANES), jnp.float32)
            net, pos = lax.fori_loop(
                0, nx,
                lambda x, s: stage(t, lambda h, i: state_b[h, i], put_r, BETAS[2], x, s),
                (z, z), unroll=2)

            def send_back(k, carry):
                dev = (k + me) % n
                deliver(result.at[t, dev % halves, pl.ds((dev // halves) * rows, rows)],
                        back.at[my_lev, my_group * per_dev + t],
                        dev, out_send.at[dev, t], out_recv.at[my_lev * groups + my_group, t])
                return carry

            lax.fori_loop(0, n, send_back, 0)
            net = jnp.sum(net, axis=1, keepdims=True)
            pos = jnp.sum(pos, axis=1, keepdims=True)
            stat[...] = jnp.where(lane == t, net, jnp.where(lane == per_dev + t, pos, stat[...]))

        def send_stat(k, carry):
            dev = (k + me) % n
            deliver(stat, stats.at[my_lev, my_group], dev, s_send.at[dev],
                    s_recv.at[my_lev * groups + my_group])
            return carry

        lax.fori_loop(0, n, send_stat, 0)

    def stat_in(k, carry):
        landed(stats.at[k // groups, k % groups], s_recv.at[k])
        return carry

    lax.fori_loop(0, targets, stat_in, 0)
    for g in range(groups):
        total = stats[0, g]
        for lv in range(1, lev):
            total = total + stats[lv, g]
        for t in range(per_dev):
            if (g * per_dev + t) * SUB < spec:
                r = total[:, t:t + 1] / total[:, per_dev + t:per_dev + t + 1]
                ratio_ref[pl.ds((g * per_dev + t) * SUB, SUB), :] = jnp.broadcast_to(r, (SUB, LANES))

    def back_in(k, carry):
        for t in range(per_dev):
            landed(back.at[k // groups, (k % groups) * per_dev + t], out_recv.at[k, t])
        return carry

    lax.fori_loop(0, targets, back_in, 0)

    for r in range(rows):
        fade = None
        for t in range(tiles):
            have = min(SUB, spec - t * SUB)
            if have <= 0:
                continue
            scale = ratio_ref[pl.ds(t * SUB, SUB), :]
            emis = emis_ref[pl.ds(t * SUB * rows + r, have, stride=rows), :]
            if have < SUB:
                emis = jnp.concatenate(
                    [emis, jnp.zeros((SUB - have, LANES), jnp.float32)], axis=0)
            value = []
            for lv in range(lev):
                right = jnp.maximum(back[lv, t, r], 0.0) * scale
                if lv == 0:
                    right = right + emis
                else:
                    right = right + coef[1, pl.ds(lv * rows + r, 1), :] * value[-1]
                value.append(right * coef[0, pl.ds(lv * rows + r, 1), :])
            mixed = [None] * lev
            mixed[lev - 1] = value[lev - 1]
            for lv in range(lev - 2, -1, -1):
                mixed[lv] = value[lv] + coef[2, pl.ds(lv * rows + r, 1), :] * mixed[lv + 1]
            if fade is None:
                fade = [None] * lev
                above = jnp.zeros((1, LANES), jnp.float32)
                for lv in range(lev - 1, -1, -1):
                    mine = mixed[lv][0:1, :]
                    fade[lv] = jnp.exp((-0.5 / lev) * (above + 0.5 * mine))
                    above = above + mine
            rate = prate[pl.ds(t * SUB, SUB), :]
            for lv in range(lev):
                val = mixed[lv] * jnp.exp(-(rate * fade[lv]))
                out_ref[pl.ds(t * SUB * stride + lv * rows + r, have, stride=stride), :] = val[0:have]

    def winds_sent(j, carry):
        dev = owner(j // groups, j % groups)
        sent(wsend.at[j // groups], dev, w_send.at[j])
        for t in range(per_dev):
            sent(send.at[j // groups, (j % groups) * per_dev + t], dev, in_send.at[j, t])
        return carry

    lax.fori_loop(0, targets, winds_sent, 0)

    @pl.when(active)
    def _():
        def results_sent(dev, carry):
            for t in range(per_dev):
                sent(result.at[t, dev % halves, pl.ds((dev // halves) * rows, rows)],
                     dev, out_send.at[dev, t])
            sent(stat, dev, s_send.at[dev])
            return carry

        lax.fori_loop(0, n, results_sent, 0)


def per_device(n, halves, conc, winds, diffusivity, emission, photo_rate):
    spec, lev, rows, lanes = conc.shape
    per = n // lev
    real = -(-spec // SUB)
    per_dev = -(-real // per)
    groups = -(-real // per_dev)
    tiles = groups * per_dev
    nx = (n // halves) * rows
    dims = (spec, lev, rows, halves, n, tiles, groups, per_dev)
    f32 = jnp.float32
    vmem = pl.BlockSpec(memory_space=pltpu.VMEM)
    dma = pltpu.SemaphoreType.DMA
    targets = lev * groups
    out = pl.pallas_call(
        functools.partial(kernel, dims),
        out_shape=jax.ShapeDtypeStruct((spec * lev * rows, lanes), f32),
        in_specs=[vmem] * 4 + [pl.BlockSpec(memory_space=pltpu.SMEM)],
        out_specs=vmem,
        scratch_shapes=[
            pltpu.VMEM((lev, tiles, rows, SUB, lanes), f32),
            pltpu.VMEM((per_dev, halves, nx + 2 * PAD, SUB, lanes), f32),
            pltpu.VMEM((halves, nx + 2 * PAD, SUB, lanes), f32),
            pltpu.VMEM((halves, nx + 2 * PAD, SUB, lanes), f32),
            pltpu.VMEM((per_dev, halves, nx, SUB, lanes), f32),
            pltpu.VMEM((lev, tiles, rows, SUB, lanes), f32),
            pltpu.VMEM((lev, 2 * rows, lanes), f32),
            pltpu.VMEM((n, 2 * rows, lanes), f32),
            pltpu.VMEM((2, halves, nx + 2 * SUB, lanes), f32),
            pltpu.VMEM((7, halves, nx, lanes), f32),
            pltpu.VMEM((7, halves, nx, lanes), f32),
            pltpu.VMEM((SUB, lanes), f32),
            pltpu.VMEM((lev, groups, SUB, lanes), f32),
            pltpu.VMEM((tiles * SUB, lanes), f32),
            pltpu.VMEM((tiles * SUB, lanes), f32),
            pltpu.VMEM((3, lev * rows, lanes), f32),
            dma((targets, per_dev)), dma((n, per_dev)),
            dma((targets,)), dma((n,)),
            dma((n, per_dev)), dma((targets, per_dev)),
            dma((n,)), dma((targets,)),
        ],
        compiler_params=pltpu.CompilerParams(collective_id=0, has_side_effects=True),
    )(
        conc.reshape(spec * lev * rows, lanes),
        winds.reshape(2 * lev * rows, lanes),
        diffusivity.reshape((lev - 1) * rows, lanes),
        emission.reshape(spec * rows, lanes),
        photo_rate,
    )
    return out.reshape(spec, lev, rows, lanes)


def solution(mesh):
    halves = mesh.shape["gy"]
    n = mesh.shape["gx"] * halves
    return jax.shard_map(
        functools.partial(per_device, n, halves),
        mesh=mesh,
        in_specs=(
            P(None, None, ("member", "gx"), "gy"),
            P(None, None, ("member", "gx"), "gy"),
            P(None, ("member", "gx"), "gy"),
            P(None, ("member", "gx"), "gy"),
            P(),
        ),
        out_specs=P(None, None, ("member", "gx"), "gy"),
        check_vma=False,
    )
```

```python
import functools

import jax
import jax.numpy as jnp
from jax import lax
from jax.experimental import pallas as pl
from jax.experimental.pallas import tpu as pltpu
from jax.sharding import PartitionSpec as P

BETAS = (1.0 / 3.0, 0.5, 1.0)
SUB = 8
LANES = 128
PAD = 3
CHUNKS = 3


def stencil_weights(km, kp):
    def face(k):
        k = k / 60.0
        a = jnp.abs(k)
        return (
            k + a,
            -8.0 * k - 5.0 * a,
            37.0 * k + 10.0 * a,
            37.0 * k - 10.0 * a,
            -8.0 * k + 5.0 * a,
            k - a,
        )

    m, p = face(km), face(kp)
    return [-m[0]] + [p[j] - m[j + 1] for j in range(5)] + [p[5]]


def kernel(dims, conc_hbm, wind_hbm, diff_hbm, emis_hbm, rate_ref, out_ref,
           conc_ref, wind_ref, diff_ref, emis_ref,
           send, state0, state_a, state_b, result, back, wsend, wrecv, cbuf, wx, wy,
           stat, stats, prate, coef,
           load_sem, in_send, in_recv, w_send, w_recv, h_send, h_recv,
           out_send, out_recv, s_send, s_recv):
    spec, lev, rows, halves, gx_n, span, tiles, chunks = dims
    n = gx_n * halves
    width = tiles // chunks
    deep = span * rows
    crews = gx_n // span
    my_gx, my_gy = lax.axis_index("gx"), lax.axis_index("gy")
    me = my_gx * halves + my_gy
    crew, seat = my_gx // span, my_gx % span
    my_lev = seat * halves + my_gy
    has_down, has_up = crew > 0, crew < crews - 1

    def where_is(dev):
        return {"gx": dev // halves, "gy": dev % halves}

    barrier = pltpu.get_barrier_semaphore()

    def greet(k, carry):
        pl.semaphore_signal(barrier, inc=1, device_id=where_is((me + k) % n),
                            device_id_type=pl.DeviceIdType.MESH)
        return carry

    lax.fori_loop(1, n, greet, 0)
    loads = [pltpu.make_async_copy(src, dst, load_sem.at[i]) for i, (src, dst) in enumerate(
        ((wind_hbm, wind_ref), (conc_hbm, conc_ref), (diff_hbm, diff_ref), (emis_hbm, emis_ref)))]
    for load in loads:
        load.start()

    stride = lev * rows
    loads[0].wait()
    for lv in range(lev):
        wsend[lv, 0:rows, :] = wind_ref[pl.ds(lv * rows, rows), :]
        wsend[lv, rows:2 * rows, :] = wind_ref[pl.ds((lev + lv) * rows, rows), :]
    loads[1].wait()
    for t in range(tiles):
        have = max(0, min(SUB, spec - t * SUB))
        for lv in range(lev):
            for r in range(rows):
                if have < SUB:
                    send[lv, t, r, :, :] = jnp.zeros((SUB, LANES), jnp.float32)
                if have > 0:
                    send[lv, t, r, 0:have, :] = conc_ref[
                        pl.ds(t * SUB * stride + lv * rows + r, have, stride=stride), :]

    pl.semaphore_wait(barrier, n - 1)

    def remote(src, dst, dev, s_sem, r_sem):
        return pltpu.make_async_remote_copy(
            src_ref=src, dst_ref=dst, send_sem=s_sem, recv_sem=r_sem,
            device_id=where_is(dev), device_id_type=pl.DeviceIdType.MESH)

    def deliver(src, dst, dev, s_sem, r_sem):
        @pl.when(dev == me)
        def _():
            pltpu.make_async_copy(src, dst, r_sem).start()

        @pl.when(dev != me)
        def _():
            remote(src, dst, dev, s_sem, r_sem).start()

    def sent(src, s_sem):
        pltpu.make_async_copy(src, src, s_sem).wait()

    def landed(dst, r_sem):
        pltpu.make_async_copy(dst, dst, r_sem).wait()

    def mate(lv):
        return (crew * span + lv // halves) * halves + lv % halves

    def tile_range(c):
        return pl.ds(c * width, width)

    sides = ((0, None, None), (1, has_up & (seat == span - 1), 0),
             (-1, has_down & (seat == 0), span + 1))

    def for_winds(act):
        for o, (shift, cond, slot) in enumerate(sides):
            at = seat + 1 if slot is None else slot
            for lv in range(lev):
                dev = mate(lv) + shift * span * halves
                if cond is None:
                    act(o, lv, dev, at)
                else:
                    pl.when(cond)(functools.partial(act, o, lv, dev, at))

    for_winds(lambda o, lv, dev, at: deliver(
        wsend.at[lv], wrecv.at[at * halves + my_gy], dev, w_send.at[o, lv],
        w_recv.at[at * halves + my_gy]))
    for c in range(chunks):
        for lv in range(lev):
            deliver(send.at[lv, tile_range(c)],
                    state0.at[tile_range(c), my_gy, pl.ds(PAD + seat * rows, rows)],
                    mate(lv), in_send.at[lv, c], in_recv.at[my_lev, c])

    lane = lax.broadcasted_iota(jnp.int32, (SUB, LANES), 1)
    states = (state0, state_a, state_b)
    blank = jnp.zeros((PAD, SUB, LANES), jnp.float32)

    @pl.when(crew == 0)
    def _():
        for buf in states:
            for t in range(tiles):
                for h in range(halves):
                    buf[t, h, 0:PAD] = blank

    @pl.when(crew == crews - 1)
    def _():
        for buf in states:
            for t in range(tiles):
                for h in range(halves):
                    buf[t, h, PAD + deep:2 * PAD + deep] = blank

    for h in range(halves):
        for c in range(2):
            cbuf[c, h, 0:SUB, :] = jnp.zeros((SUB, LANES), jnp.float32)
            cbuf[c, h, SUB + deep:2 * SUB + deep, :] = jnp.zeros((SUB, LANES), jnp.float32)

    def wind_in(slot):
        for h in range(halves):
            landed(wrecv.at[slot * halves + h], w_recv.at[slot * halves + h])
            for c in range(2):
                base = SUB + (slot - 1) * rows
                cbuf[c, h, base:base + rows, :] = wrecv[
                    slot * halves + h, c * rows:(c + 1) * rows, :]

    for slot in range(1, span + 1):
        wind_in(slot)
    pl.when(has_down)(lambda: wind_in(0))
    pl.when(has_up)(lambda: wind_in(span + 1))
    for x0 in range(0, deep, SUB):
        for h in range(halves):
            here = cbuf[0, h, SUB + x0:SUB + x0 + SUB, :]
            left = cbuf[0, h, SUB + x0 - 1:SUB + x0 - 1 + SUB, :]
            right = cbuf[0, h, SUB + x0 + 1:SUB + x0 + 1 + SUB, :]
            for j, w in enumerate(stencil_weights(0.5 * (left + here), 0.5 * (here + right))):
                wx[j, h, x0:x0 + SUB, :] = w
        cy = [cbuf[1, h, SUB + x0:SUB + x0 + SUB, :] for h in range(halves)]
        zer = jnp.zeros((SUB, LANES), jnp.float32)
        for h in range(halves):
            nxt = pltpu.roll(cy[h + 1], LANES - 1, 1) if h + 1 < halves else zer
            prv = pltpu.roll(cy[h - 1], 1, 1) if h > 0 else zer
            up = jnp.where(lane < LANES - 1, pltpu.roll(cy[h], LANES - 1, 1), nxt)
            down = jnp.where(lane >= 1, pltpu.roll(cy[h], 1, 1), prv)
            ws = stencil_weights(0.5 * (down + cy[h]), 0.5 * (cy[h] + up))
            for j, w in enumerate(ws):
                d = j - 3
                if d > 0 and h == halves - 1:
                    w = jnp.where(lane < LANES - d, w, 0.0)
                if d < 0 and h == 0:
                    w = jnp.where(lane >= -d, w, 0.0)
                wy[j, h, x0:x0 + SUB, :] = w

    def halo(s, c, d):
        buf, own = states[s], tile_range(c)
        first, land = (deep, 0) if d == 0 else (PAD, PAD + deep)
        return remote(
            buf.at[own, :, pl.ds(first, PAD)], buf.at[own, :, pl.ds(land, PAD)],
            me + (span * halves if d == 0 else -span * halves),
            h_send.at[s, c, d], h_recv.at[s, c, d])

    def start_halo(s, c):
        pl.when(has_up)(lambda: halo(s, c, 0).start())
        pl.when(has_down)(lambda: halo(s, c, 1).start())

    def wait_halo(s, c):
        own = tile_range(c)
        pl.when(has_down)(lambda: landed(states[s].at[own, :, pl.ds(0, PAD)], h_recv.at[s, c, 0]))
        pl.when(has_up)(lambda: landed(
            states[s].at[own, :, pl.ds(PAD + deep, PAD)], h_recv.at[s, c, 1]))

    for c in range(chunks):
        for lv in range(lev):
            landed(state0.at[tile_range(c), lv % halves, pl.ds(PAD + (lv // halves) * rows, rows)],
                   in_recv.at[lv, c])
        start_halo(0, c)

    def stage(c, src, dst, off, beta, x, sums):
        wxs = [[wx[j, h, pl.ds(x, 1), :] * beta for j in range(7)] for h in range(halves)]
        wys = [[wy[j, h, pl.ds(x, 1), :] * beta for j in range(7)] for h in range(halves)]
        out = []
        for i in range(width):
            t = c * width + i
            partial, new = [], []
            for h in range(halves):
                acc = wxs[h][0] * src[t, h, x]
                for j in range(1, 7):
                    acc = acc + wxs[h][j] * src[t, h, x + j]
                mid = src[t, h, x + PAD]
                p = mid - acc
                partial.append(p)
                start = mid if src is state0 else state0[t, h, x + PAD]
                new.append(start - acc - wys[h][3] * p)
            for d in (1, 2, 3):
                up = [pltpu.roll(p, LANES - d, 1) for p in partial]
                down = [pltpu.roll(p, d, 1) for p in partial]
                for h in range(halves):
                    u = up[h] if h == halves - 1 else jnp.where(lane < LANES - d, up[h], up[h + 1])
                    w = down[h] if h == 0 else jnp.where(lane >= d, down[h], down[h - 1])
                    new[h] = new[h] - (wys[h][3 + d] * u + wys[h][3 - d] * w)
            for h in range(halves):
                dst[t, h, x + off] = new[h]
            if sums is not None:
                net, pos = sums[2 * i], sums[2 * i + 1]
                for v in new:
                    net, pos = net + v, pos + jnp.maximum(v, 0.0)
                out += [net, pos]
        return tuple(out)

    stat[...] = jnp.zeros((SUB, LANES), jnp.float32)
    for s in range(3):
        for c in range(chunks):
            wait_halo(s, c)
            if s < 2:

                @pl.loop(0, deep)
                def _(x):
                    stage(c, states[s], states[s + 1], PAD, BETAS[s], x, None)

                start_halo(s + 1, c)
                continue
            z = jnp.zeros((SUB, LANES), jnp.float32)
            sums = lax.fori_loop(
                0, deep, lambda x, v: stage(c, states[s], result, 0, BETAS[s], x, v),
                (z,) * (2 * width))
            for lv in range(lev):
                deliver(result.at[tile_range(c), lv % halves, pl.ds((lv // halves) * rows, rows)],
                        back.at[my_lev, tile_range(c)], mate(lv),
                        out_send.at[lv, c], out_recv.at[my_lev, c])
            acc = stat[...]
            for i in range(width):
                t = c * width + i
                net = jnp.sum(sums[2 * i], axis=1, keepdims=True)
                pos = jnp.sum(sums[2 * i + 1], axis=1, keepdims=True)
                acc = jnp.where(lane == t, net, jnp.where(lane == tiles + t, pos, acc))
            stat[...] = acc

    def send_stat(k, carry):
        dev = (k + me) % n
        deliver(stat, stats.at[me], dev, s_send.at[dev], s_recv.at[me])
        return carry

    lax.fori_loop(0, n, send_stat, 0)

    sub = lax.broadcasted_iota(jnp.int32, (SUB, LANES), 0)
    for t in range(tiles):
        tile = jnp.zeros((SUB, LANES), jnp.float32)
        for i in range(SUB):
            if t * SUB + i < spec:
                tile = jnp.where(sub == i, rate_ref[t * SUB + i], tile)
        prate[pl.ds(t * SUB, SUB), :] = tile
    loads[2].wait()
    loads[3].wait()
    ks = [diff_ref[lv] for lv in range(lev - 1)]
    zero = jnp.zeros((rows, LANES), jnp.float32)
    lower = [zero] + ks
    upper = ks + [zero]
    prev = None
    for lv in range(lev):
        pivot = 1.0 + lower[lv] + upper[lv]
        if lv:
            pivot = pivot + lower[lv] * prev
        inv = 1.0 / pivot
        prev = -upper[lv] * inv
        coef[0, pl.ds(lv * rows, rows), :] = inv
        coef[1, pl.ds(lv * rows, rows), :] = lower[lv]
        coef[2, pl.ds(lv * rows, rows), :] = -prev

    def stat_in(k, carry):
        landed(stats.at[k], s_recv.at[k])
        return carry

    for c in range(chunks):
        for lv in range(lev):
            landed(back.at[lv, tile_range(c)], out_recv.at[lv, c])
    lax.fori_loop(0, n, stat_in, 0)
    total = stats[0]
    for k in range(1, n):
        total = total + stats[k]

    fades = [None] * rows
    for t in range(tiles):
        have = min(SUB, spec - t * SUB)
        if have <= 0:
            continue
        scale = jnp.broadcast_to(
            total[:, t:t + 1] / total[:, tiles + t:tiles + t + 1], (SUB, LANES))
        rate = prate[pl.ds(t * SUB, SUB), :]
        for r in range(rows):
            emis = emis_ref[pl.ds(t * SUB * rows + r, have, stride=rows), :]
            if have < SUB:
                emis = jnp.concatenate(
                    [emis, jnp.zeros((SUB - have, LANES), jnp.float32)], axis=0)
            value = []
            for lv in range(lev):
                right = jnp.maximum(back[lv, t, r], 0.0) * scale
                if lv == 0:
                    right = right + emis
                else:
                    right = right + coef[1, pl.ds(lv * rows + r, 1), :] * value[-1]
                value.append(right * coef[0, pl.ds(lv * rows + r, 1), :])
            mixed = [None] * lev
            mixed[lev - 1] = value[lev - 1]
            for lv in range(lev - 2, -1, -1):
                mixed[lv] = value[lv] + coef[2, pl.ds(lv * rows + r, 1), :] * mixed[lv + 1]
            if t == 0:
                fade = [None] * lev
                above = jnp.zeros((1, LANES), jnp.float32)
                for lv in range(lev - 1, -1, -1):
                    mine = mixed[lv][0:1, :]
                    fade[lv] = jnp.exp((-0.5 / lev) * (above + 0.5 * mine))
                    above = above + mine
                fades[r] = fade
            for lv in range(lev):
                val = mixed[lv] * jnp.exp(-(rate * fades[r][lv]))
                out_ref[pl.ds(t * SUB * stride + lv * rows + r, have, stride=stride), :] = val[0:have]

    def wind_sent(o, lv, dev, at):
        pl.when(dev != me)(lambda: sent(wsend.at[lv], w_send.at[o, lv]))

    for_winds(wind_sent)
    for lv in range(lev):

        @pl.when(lv != my_lev)
        def _():
            for c in range(chunks):
                sent(send.at[lv, tile_range(c)], in_send.at[lv, c])
                sent(result.at[tile_range(c), lv % halves, pl.ds((lv // halves) * rows, rows)],
                     out_send.at[lv, c])

    for s in range(3):
        for c in range(chunks):
            own = tile_range(c)
            pl.when(has_up)(lambda: sent(states[s].at[own, :, pl.ds(deep, PAD)], h_send.at[s, c, 0]))
            pl.when(has_down)(lambda: sent(states[s].at[own, :, pl.ds(PAD, PAD)], h_send.at[s, c, 1]))

    def stat_sent(k, carry):
        sent(stat, s_send.at[(k + me) % n])
        return carry

    lax.fori_loop(1, n, stat_sent, 0)


def per_device(gx_n, halves, conc, winds, diffusivity, emission, photo_rate):
    spec, lev, rows, lanes = conc.shape
    span = lev // halves
    assert span * halves == lev and gx_n % span == 0
    n = gx_n * halves
    real = -(-spec // SUB)
    chunks = CHUNKS
    width = -(-real // chunks)
    tiles = chunks * width
    deep = span * rows
    dims = (spec, lev, rows, halves, gx_n, span, tiles, chunks)
    f32 = jnp.float32
    hbm = pl.BlockSpec(memory_space=pl.ANY)
    dma = pltpu.SemaphoreType.DMA
    slots = (span + 2) * halves
    out = pl.pallas_call(
        functools.partial(kernel, dims),
        out_shape=jax.ShapeDtypeStruct((spec * lev * rows, lanes), f32),
        in_specs=[hbm] * 4 + [pl.BlockSpec(memory_space=pltpu.SMEM)],
        out_specs=pl.BlockSpec(memory_space=pltpu.VMEM),
        scratch_shapes=[
            pltpu.VMEM((spec * lev * rows, lanes), f32),
            pltpu.VMEM((2 * lev * rows, lanes), f32),
            pltpu.VMEM((lev - 1, rows, lanes), f32),
            pltpu.VMEM((spec * rows, lanes), f32),
            pltpu.VMEM((lev, tiles, rows, SUB, lanes), f32),
            pltpu.VMEM((tiles, halves, deep + 2 * PAD, SUB, lanes), f32),
            pltpu.VMEM((tiles, halves, deep + 2 * PAD, SUB, lanes), f32),
            pltpu.VMEM((tiles, halves, deep + 2 * PAD, SUB, lanes), f32),
            pltpu.VMEM((tiles, halves, deep, SUB, lanes), f32),
            pltpu.VMEM((lev, tiles, rows, SUB, lanes), f32),
            pltpu.VMEM((lev, 2 * rows, lanes), f32),
            pltpu.VMEM((slots, 2 * rows, lanes), f32),
            pltpu.VMEM((2, halves, deep + 2 * SUB, lanes), f32),
            pltpu.VMEM((7, halves, deep, lanes), f32),
            pltpu.VMEM((7, halves, deep, lanes), f32),
            pltpu.VMEM((SUB, lanes), f32),
            pltpu.VMEM((n, SUB, lanes), f32),
            pltpu.VMEM((tiles * SUB, lanes), f32),
            pltpu.VMEM((3, lev * rows, lanes), f32),
            dma((4,)),
            dma((lev, chunks)), dma((lev, chunks)),
            dma((3, lev)), dma((slots,)),
            dma((3, chunks, 2)), dma((3, chunks, 2)),
            dma((lev, chunks)), dma((lev, chunks)),
            dma((n,)), dma((n,)),
        ],
        compiler_params=pltpu.CompilerParams(collective_id=0, has_side_effects=True),
    )(
        conc.reshape(spec * lev * rows, lanes),
        winds.reshape(2 * lev * rows, lanes),
        diffusivity,
        emission.reshape(spec * rows, lanes),
        photo_rate,
    )
    return out.reshape(spec, lev, rows, lanes)


def solution(mesh):
    halves = mesh.shape["gy"]
    gx_n = mesh.shape["gx"]
    return jax.shard_map(
        functools.partial(per_device, gx_n, halves),
        mesh=mesh,
        in_specs=(
            P(None, None, ("member", "gx"), "gy"),
            P(None, None, ("member", "gx"), "gy"),
            P(None, ("member", "gx"), "gy"),
            P(None, ("member", "gx"), "gy"),
            P(),
        ),
        out_specs=P(None, None, ("member", "gx"), "gy"),
        check_vma=False,
    )
```

```python
import functools

import jax
import jax.numpy as jnp
from jax import lax
from jax.experimental import pallas as pl
from jax.experimental.pallas import tpu as pltpu
from jax.sharding import PartitionSpec as P

BETAS = (1.0 / 3.0, 0.5, 1.0)
SUB = 8
LANES = 128
PAD = 3
CHUNKS = 3


def stencil_weights(km, kp):
    def face(k):
        k = k / 60.0
        a = jnp.abs(k)
        return (
            k + a,
            -8.0 * k - 5.0 * a,
            37.0 * k + 10.0 * a,
            37.0 * k - 10.0 * a,
            -8.0 * k + 5.0 * a,
            k - a,
        )

    m, p = face(km), face(kp)
    return [-m[0]] + [p[j] - m[j + 1] for j in range(5)] + [p[5]]


def kernel(dims, conc_hbm, wind_hbm, diff_hbm, emis_hbm, rate_ref, out_hbm,
           conc_ref, wind_ref, diff_ref, emis_ref,
           send, state0, state_a, state_b, result, back, wsend, wrecv, cbuf, wx, wy,
           stat, stats, prate, coef,
           load_sem, in_send, in_recv, w_send, w_recv, h_send, h_recv,
           out_send, out_recv, s_send, s_recv, out_ref, store_sem):
    spec, lev, rows, halves, gx_n, span, tiles, chunks = dims
    n = gx_n * halves
    width = tiles // chunks
    deep = span * rows
    crews = gx_n // span
    my_gx, my_gy = lax.axis_index("gx"), lax.axis_index("gy")
    me = my_gx * halves + my_gy
    crew, seat = my_gx // span, my_gx % span
    my_lev = seat * halves + my_gy
    has_down, has_up = crew > 0, crew < crews - 1

    def where_is(dev):
        return {"gx": dev // halves, "gy": dev % halves}

    barrier = pltpu.get_barrier_semaphore()

    def greet(k, carry):
        pl.semaphore_signal(barrier, inc=1, device_id=where_is((me + k) % n),
                            device_id_type=pl.DeviceIdType.MESH)
        return carry

    lax.fori_loop(1, n, greet, 0)
    loads = [pltpu.make_async_copy(src, dst, load_sem.at[i]) for i, (src, dst) in enumerate(
        ((wind_hbm, wind_ref), (conc_hbm, conc_ref), (diff_hbm, diff_ref), (emis_hbm, emis_ref)))]
    for load in loads:
        load.start()

    stride = lev * rows
    loads[0].wait()
    for lv in range(lev):
        wsend[lv, 0:rows, :] = wind_ref[pl.ds(lv * rows, rows), :]
        wsend[lv, rows:2 * rows, :] = wind_ref[pl.ds((lev + lv) * rows, rows), :]
    loads[1].wait()
    for t in range(tiles):
        have = max(0, min(SUB, spec - t * SUB))
        for lv in range(lev):
            for r in range(rows):
                if have < SUB:
                    send[lv, t, r, :, :] = jnp.zeros((SUB, LANES), jnp.float32)
                if have > 0:
                    send[lv, t, r, 0:have, :] = conc_ref[
                        pl.ds(t * SUB * stride + lv * rows + r, have, stride=stride), :]

    pl.semaphore_wait(barrier, n - 1)

    def remote(src, dst, dev, s_sem, r_sem):
        return pltpu.make_async_remote_copy(
            src_ref=src, dst_ref=dst, send_sem=s_sem, recv_sem=r_sem,
            device_id=where_is(dev), device_id_type=pl.DeviceIdType.MESH)

    def deliver(src, dst, dev, s_sem, r_sem):
        @pl.when(dev == me)
        def _():
            pltpu.make_async_copy(src, dst, r_sem).start()

        @pl.when(dev != me)
        def _():
            remote(src, dst, dev, s_sem, r_sem).start()

    def sent(src, s_sem):
        pltpu.make_async_copy(src, src, s_sem).wait()

    def landed(dst, r_sem):
        pltpu.make_async_copy(dst, dst, r_sem).wait()

    def mate(lv):
        return (crew * span + lv // halves) * halves + lv % halves

    def tile_range(c):
        return pl.ds(c * width, width)

    sides = ((0, None, None), (1, has_up & (seat == span - 1), 0),
             (-1, has_down & (seat == 0), span + 1))

    def for_winds(act):
        for o, (shift, cond, slot) in enumerate(sides):
            at = seat + 1 if slot is None else slot
            for lv in range(lev):
                dev = mate(lv) + shift * span * halves
                if cond is None:
                    act(o, lv, dev, at)
                else:
                    pl.when(cond)(functools.partial(act, o, lv, dev, at))

    for_winds(lambda o, lv, dev, at: deliver(
        wsend.at[lv], wrecv.at[at * halves + my_gy], dev, w_send.at[o, lv],
        w_recv.at[at * halves + my_gy]))
    for c in range(chunks):
        for lv in range(lev):
            deliver(send.at[lv, tile_range(c)],
                    state0.at[tile_range(c), my_gy, pl.ds(PAD + seat * rows, rows)],
                    mate(lv), in_send.at[lv, c], in_recv.at[my_lev, c])

    lane = lax.broadcasted_iota(jnp.int32, (SUB, LANES), 1)
    states = (state0, state_a, state_b)
    blank = jnp.zeros((PAD, SUB, LANES), jnp.float32)

    @pl.when(crew == 0)
    def _():
        for buf in states:
            for t in range(tiles):
                for h in range(halves):
                    buf[t, h, 0:PAD] = blank

    @pl.when(crew == crews - 1)
    def _():
        for buf in states:
            for t in range(tiles):
                for h in range(halves):
                    buf[t, h, PAD + deep:2 * PAD + deep] = blank

    for h in range(halves):
        for c in range(2):
            cbuf[c, h, 0:SUB, :] = jnp.zeros((SUB, LANES), jnp.float32)
            cbuf[c, h, SUB + deep:2 * SUB + deep, :] = jnp.zeros((SUB, LANES), jnp.float32)

    def wind_in(slot):
        for h in range(halves):
            landed(wrecv.at[slot * halves + h], w_recv.at[slot * halves + h])
            for c in range(2):
                base = SUB + (slot - 1) * rows
                cbuf[c, h, base:base + rows, :] = wrecv[
                    slot * halves + h, c * rows:(c + 1) * rows, :]

    for slot in range(1, span + 1):
        wind_in(slot)
    pl.when(has_down)(lambda: wind_in(0))
    pl.when(has_up)(lambda: wind_in(span + 1))
    for x0 in range(0, deep, SUB):
        for h in range(halves):
            here = cbuf[0, h, SUB + x0:SUB + x0 + SUB, :]
            left = cbuf[0, h, SUB + x0 - 1:SUB + x0 - 1 + SUB, :]
            right = cbuf[0, h, SUB + x0 + 1:SUB + x0 + 1 + SUB, :]
            for j, w in enumerate(stencil_weights(0.5 * (left + here), 0.5 * (here + right))):
                wx[j, h, x0:x0 + SUB, :] = w
        cy = [cbuf[1, h, SUB + x0:SUB + x0 + SUB, :] for h in range(halves)]
        zer = jnp.zeros((SUB, LANES), jnp.float32)
        for h in range(halves):
            nxt = pltpu.roll(cy[h + 1], LANES - 1, 1) if h + 1 < halves else zer
            prv = pltpu.roll(cy[h - 1], 1, 1) if h > 0 else zer
            up = jnp.where(lane < LANES - 1, pltpu.roll(cy[h], LANES - 1, 1), nxt)
            down = jnp.where(lane >= 1, pltpu.roll(cy[h], 1, 1), prv)
            ws = stencil_weights(0.5 * (down + cy[h]), 0.5 * (cy[h] + up))
            for j, w in enumerate(ws):
                d = j - 3
                if d > 0 and h == halves - 1:
                    w = jnp.where(lane < LANES - d, w, 0.0)
                if d < 0 and h == 0:
                    w = jnp.where(lane >= -d, w, 0.0)
                wy[j, h, x0:x0 + SUB, :] = w

    def halo(s, c, d):
        buf, own = states[s], tile_range(c)
        first, land = (deep, 0) if d == 0 else (PAD, PAD + deep)
        return remote(
            buf.at[own, :, pl.ds(first, PAD)], buf.at[own, :, pl.ds(land, PAD)],
            me + (span * halves if d == 0 else -span * halves),
            h_send.at[s, c, d], h_recv.at[s, c, d])

    def start_halo(s, c):
        pl.when(has_up)(lambda: halo(s, c, 0).start())
        pl.when(has_down)(lambda: halo(s, c, 1).start())

    def wait_halo(s, c):
        own = tile_range(c)
        pl.when(has_down)(lambda: landed(states[s].at[own, :, pl.ds(0, PAD)], h_recv.at[s, c, 0]))
        pl.when(has_up)(lambda: landed(
            states[s].at[own, :, pl.ds(PAD + deep, PAD)], h_recv.at[s, c, 1]))

    for c in range(chunks):
        for lv in range(lev):
            landed(state0.at[tile_range(c), lv % halves, pl.ds(PAD + (lv // halves) * rows, rows)],
                   in_recv.at[lv, c])
        start_halo(0, c)

    def stage(c, src, dst, off, beta, x, sums):
        wxs = [[wx[j, h, pl.ds(x, 1), :] * beta for j in range(7)] for h in range(halves)]
        wys = [[wy[j, h, pl.ds(x, 1), :] * beta for j in range(7)] for h in range(halves)]
        out = []
        for i in range(width):
            t = c * width + i
            partial, new = [], []
            for h in range(halves):
                acc = wxs[h][0] * src[t, h, x]
                for j in range(1, 7):
                    acc = acc + wxs[h][j] * src[t, h, x + j]
                mid = src[t, h, x + PAD]
                p = mid - acc
                partial.append(p)
                start = mid if src is state0 else state0[t, h, x + PAD]
                new.append(start - acc - wys[h][3] * p)
            for d in (1, 2, 3):
                up = [pltpu.roll(p, LANES - d, 1) for p in partial]
                down = [pltpu.roll(p, d, 1) for p in partial]
                for h in range(halves):
                    u = up[h] if h == halves - 1 else jnp.where(lane < LANES - d, up[h], up[h + 1])
                    w = down[h] if h == 0 else jnp.where(lane >= d, down[h], down[h - 1])
                    new[h] = new[h] - (wys[h][3 + d] * u + wys[h][3 - d] * w)
            for h in range(halves):
                dst[t, h, x + off] = new[h]
            if sums is not None:
                net, pos = sums[2 * i], sums[2 * i + 1]
                for v in new:
                    net, pos = net + v, pos + jnp.maximum(v, 0.0)
                out += [net, pos]
        return tuple(out)

    stat[...] = jnp.zeros((SUB, LANES), jnp.float32)
    for s in range(3):
        for c in range(chunks):
            wait_halo(s, c)
            if s < 2:

                @pl.loop(0, deep)
                def _(x):
                    stage(c, states[s], states[s + 1], PAD, BETAS[s], x, None)

                start_halo(s + 1, c)
                continue
            z = jnp.zeros((SUB, LANES), jnp.float32)
            sums = lax.fori_loop(
                0, deep, lambda x, v: stage(c, states[s], result, 0, BETAS[s], x, v),
                (z,) * (2 * width))
            for lv in range(lev):
                deliver(result.at[tile_range(c), lv % halves, pl.ds((lv // halves) * rows, rows)],
                        back.at[my_lev, tile_range(c)], mate(lv),
                        out_send.at[lv, c], out_recv.at[my_lev, c])
            acc = stat[...]
            for i in range(width):
                t = c * width + i
                net = jnp.sum(sums[2 * i], axis=1, keepdims=True)
                pos = jnp.sum(sums[2 * i + 1], axis=1, keepdims=True)
                acc = jnp.where(lane == t, net, jnp.where(lane == tiles + t, pos, acc))
            stat[...] = acc

    def send_stat(k, carry):
        dev = (k + me) % n
        deliver(stat, stats.at[me], dev, s_send.at[dev], s_recv.at[me])
        return carry

    lax.fori_loop(0, n, send_stat, 0)

    sub = lax.broadcasted_iota(jnp.int32, (SUB, LANES), 0)
    for t in range(tiles):
        tile = jnp.zeros((SUB, LANES), jnp.float32)
        for i in range(SUB):
            if t * SUB + i < spec:
                tile = jnp.where(sub == i, rate_ref[t * SUB + i], tile)
        prate[pl.ds(t * SUB, SUB), :] = tile
    loads[2].wait()
    loads[3].wait()
    ks = [diff_ref[lv] for lv in range(lev - 1)]
    zero = jnp.zeros((rows, LANES), jnp.float32)
    lower = [zero] + ks
    upper = ks + [zero]
    prev = None
    for lv in range(lev):
        pivot = 1.0 + lower[lv] + upper[lv]
        if lv:
            pivot = pivot + lower[lv] * prev
        inv = 1.0 / pivot
        prev = -upper[lv] * inv
        coef[0, pl.ds(lv * rows, rows), :] = inv
        coef[1, pl.ds(lv * rows, rows), :] = lower[lv]
        coef[2, pl.ds(lv * rows, rows), :] = -prev

    def stat_in(k, carry):
        landed(stats.at[k], s_recv.at[k])
        return carry

    for c in range(chunks):
        for lv in range(lev):
            landed(back.at[lv, tile_range(c)], out_recv.at[lv, c])
    lax.fori_loop(0, n, stat_in, 0)
    total = stats[0]
    for k in range(1, n):
        total = total + stats[k]

    fades = [None] * rows
    stores = []
    for t in range(tiles):
        have = min(SUB, spec - t * SUB)
        if have <= 0:
            continue
        scale = jnp.broadcast_to(
            total[:, t:t + 1] / total[:, tiles + t:tiles + t + 1], (SUB, LANES))
        rate = prate[pl.ds(t * SUB, SUB), :]
        for r in range(rows):
            emis = emis_ref[pl.ds(t * SUB * rows + r, have, stride=rows), :]
            if have < SUB:
                emis = jnp.concatenate(
                    [emis, jnp.zeros((SUB - have, LANES), jnp.float32)], axis=0)
            value = []
            for lv in range(lev):
                right = jnp.maximum(back[lv, t, r], 0.0) * scale
                if lv == 0:
                    right = right + emis
                else:
                    right = right + coef[1, pl.ds(lv * rows + r, 1), :] * value[-1]
                value.append(right * coef[0, pl.ds(lv * rows + r, 1), :])
            mixed = [None] * lev
            mixed[lev - 1] = value[lev - 1]
            for lv in range(lev - 2, -1, -1):
                mixed[lv] = value[lv] + coef[2, pl.ds(lv * rows + r, 1), :] * mixed[lv + 1]
            if t == 0:
                fade = [None] * lev
                above = jnp.zeros((1, LANES), jnp.float32)
                for lv in range(lev - 1, -1, -1):
                    mine = mixed[lv][0:1, :]
                    fade[lv] = jnp.exp((-0.5 / lev) * (above + 0.5 * mine))
                    above = above + mine
                fades[r] = fade
            for lv in range(lev):
                val = mixed[lv] * jnp.exp(-(rate * fades[r][lv]))
                out_ref[pl.ds(t * SUB * stride + lv * rows + r, have, stride=stride), :] = val[0:have]
        done = pl.ds(t * SUB * stride, have * stride)
        stores.append(pltpu.make_async_copy(out_ref.at[done], out_hbm.at[done], store_sem.at[t]))
        stores[-1].start()

    def wind_sent(o, lv, dev, at):
        pl.when(dev != me)(lambda: sent(wsend.at[lv], w_send.at[o, lv]))

    for_winds(wind_sent)
    for lv in range(lev):

        @pl.when(lv != my_lev)
        def _():
            for c in range(chunks):
                sent(send.at[lv, tile_range(c)], in_send.at[lv, c])
                sent(result.at[tile_range(c), lv % halves, pl.ds((lv // halves) * rows, rows)],
                     out_send.at[lv, c])

    for s in range(3):
        for c in range(chunks):
            own = tile_range(c)
            pl.when(has_up)(lambda: sent(states[s].at[own, :, pl.ds(deep, PAD)], h_send.at[s, c, 0]))
            pl.when(has_down)(lambda: sent(states[s].at[own, :, pl.ds(PAD, PAD)], h_send.at[s, c, 1]))

    def stat_sent(k, carry):
        sent(stat, s_send.at[(k + me) % n])
        return carry

    lax.fori_loop(1, n, stat_sent, 0)
    for store in stores:
        store.wait()


def per_device(gx_n, halves, conc, winds, diffusivity, emission, photo_rate):
    spec, lev, rows, lanes = conc.shape
    span = lev // halves
    assert span * halves == lev and gx_n % span == 0
    n = gx_n * halves
    real = -(-spec // SUB)
    chunks = CHUNKS
    width = -(-real // chunks)
    tiles = chunks * width
    deep = span * rows
    dims = (spec, lev, rows, halves, gx_n, span, tiles, chunks)
    f32 = jnp.float32
    hbm = pl.BlockSpec(memory_space=pl.ANY)
    dma = pltpu.SemaphoreType.DMA
    slots = (span + 2) * halves
    out = pl.pallas_call(
        functools.partial(kernel, dims),
        out_shape=jax.ShapeDtypeStruct((spec * lev * rows, lanes), f32),
        in_specs=[hbm] * 4 + [pl.BlockSpec(memory_space=pltpu.SMEM)],
        out_specs=hbm,
        scratch_shapes=[
            pltpu.VMEM((spec * lev * rows, lanes), f32),
            pltpu.VMEM((2 * lev * rows, lanes), f32),
            pltpu.VMEM((lev - 1, rows, lanes), f32),
            pltpu.VMEM((spec * rows, lanes), f32),
            pltpu.VMEM((lev, tiles, rows, SUB, lanes), f32),
            pltpu.VMEM((tiles, halves, deep + 2 * PAD, SUB, lanes), f32),
            pltpu.VMEM((tiles, halves, deep + 2 * PAD, SUB, lanes), f32),
            pltpu.VMEM((tiles, halves, deep + 2 * PAD, SUB, lanes), f32),
            pltpu.VMEM((tiles, halves, deep, SUB, lanes), f32),
            pltpu.VMEM((lev, tiles, rows, SUB, lanes), f32),
            pltpu.VMEM((lev, 2 * rows, lanes), f32),
            pltpu.VMEM((slots, 2 * rows, lanes), f32),
            pltpu.VMEM((2, halves, deep + 2 * SUB, lanes), f32),
            pltpu.VMEM((7, halves, deep, lanes), f32),
            pltpu.VMEM((7, halves, deep, lanes), f32),
            pltpu.VMEM((SUB, lanes), f32),
            pltpu.VMEM((n, SUB, lanes), f32),
            pltpu.VMEM((tiles * SUB, lanes), f32),
            pltpu.VMEM((3, lev * rows, lanes), f32),
            dma((4,)),
            dma((lev, chunks)), dma((lev, chunks)),
            dma((3, lev)), dma((slots,)),
            dma((3, chunks, 2)), dma((3, chunks, 2)),
            dma((lev, chunks)), dma((lev, chunks)),
            dma((n,)), dma((n,)),
            pltpu.VMEM((spec * lev * rows, lanes), f32), dma((tiles,)),
        ],
        compiler_params=pltpu.CompilerParams(collective_id=0, has_side_effects=True),
    )(
        conc.reshape(spec * lev * rows, lanes),
        winds.reshape(2 * lev * rows, lanes),
        diffusivity,
        emission.reshape(spec * rows, lanes),
        photo_rate,
    )
    return out.reshape(spec, lev, rows, lanes)


def solution(mesh):
    halves = mesh.shape["gy"]
    gx_n = mesh.shape["gx"]
    return jax.shard_map(
        functools.partial(per_device, gx_n, halves),
        mesh=mesh,
        in_specs=(
            P(None, None, ("member", "gx"), "gy"),
            P(None, None, ("member", "gx"), "gy"),
            P(None, ("member", "gx"), "gy"),
            P(None, ("member", "gx"), "gy"),
            P(),
        ),
        out_specs=P(None, None, ("member", "gx"), "gy"),
        check_vma=False,
    )
```
